256 devices in a mesh: leaf: 4 (over y_hi, core), grid: 64 (over z, x, y_lo).
Axes of the slice: x: 4, y: 4 (y_hi: 2, y_lo: 2; y = y_hi * 2 + y_lo), z: 8, core: 2. Of those that a mesh axis runs over, the one named last changes fastest.
Arguments:
- ainv_sep: bfloat16 [4, 16384, 16384], P('leaf', 'grid'), may hold values from -6 to 6
- l_panel: bfloat16 [4, 16384, 512], P('leaf', 'grid'), may hold values from -0.046875 to 0.046875
- block_mask: int32 [4, 1, 32], P('leaf'), may hold values 0 or 1
- owner: int32 [4, 32], P('leaf'), may hold values 0 or 1
- dinv: float32 [4, 512, 512], P('leaf', 'grid'), may hold values from -6 to 6
Outputs:
- ainv_panel: bfloat16 [4, 16384, 512], P('leaf', 'grid')
- ainv_upper: bfloat16 [4, 512, 16384], P('leaf', 'grid')
- ainv_diag: float32 [4, 512, 512], P('leaf', 'grid')
The draws below stay inside these ranges and needn't reach their ends.
All inputs are finite; a program needn't handle non-finite values. No bound on the sum of `block_mask` or of `owner` on one device may be relied on, other than what follows from the above.
Results may differ from the reference program's by a relative error of at most 0.0019.
Values may be sent and summed in bfloat16 or wider, within the bound.
A program may use at most 128 MiB of HBM per device.

```python
import jax
import jax.numpy as jnp
from jax import lax

B = 512
NSUP = 1
SEP = 16384
NB = 32
W = 512
N_LEAF = 4


def with_ends(drawn, key, least, high):
    place = [jax.random.randint(jax.random.fold_in(key, axis), (), 0, length) for axis, length in enumerate(drawn.shape)]
    longest = drawn.shape.index(max(drawn.shape))
    beside = place[:longest] + [(place[longest] + 1) % drawn.shape[longest]] + place[longest + 1:]
    return drawn.at[tuple(place)].set(least).at[tuple(beside)].set(high)


def shard_levels(rng, shape, split, least, largest):
    level, own = 1.0, jax.random.fold_in(rng, 6)
    for position, parts in split:
        draws = jnp.exp(jax.random.uniform(jax.random.fold_in(own, position), (parts,), jnp.float32, least / len(split), largest / len(split)))
        level = level * jnp.repeat(draws, shape[position] // parts).reshape([-1 if axis == position else 1 for axis in range(len(shape))])
    return level


def normal_values(rng, shape, deviation, limit, pieces=(), dtype=jnp.bfloat16):
    array = deviation * jax.random.normal(rng, shape, jnp.float32)
    if pieces:
        array = array * shard_levels(rng, shape, pieces, -0.22, 0.18)
    return jnp.clip(array, -limit, limit).astype(dtype)


def setup_inputs(seed: int = 0) -> dict:
    key_list = jax.random.split(jax.random.key(seed), 6)
    ainv_sep = normal_values(key_list[0], (N_LEAF, SEP, SEP), 1.0, 6.0, ((0, 4), (1, 64)))
    l_panel = normal_values(key_list[1], (N_LEAF, SEP, W), SEP ** -0.5, 0.046875, ((0, 4), (1, 64)))
    block_mask = with_ends((jax.random.randint(key_list[2], (N_LEAF, NSUP, NB), 0, 3) < 2).astype(jnp.int32), jax.random.fold_in(key_list[2], 1), 0, 1)
    owner = with_ends((jax.random.randint(key_list[3], (N_LEAF, NB), 0, 2) < 1).astype(jnp.int32), jax.random.fold_in(key_list[3], 1), 0, 1)
    dinv = normal_values(key_list[4], (N_LEAF, W, B), 1.0, 6.0, ((0, 4), (1, 64)), jnp.float32)
    return dict(ainv_sep=ainv_sep, l_panel=l_panel, block_mask=block_mask, owner=owner, dinv=dinv)


def reference(ainv_sep, l_panel, block_mask, owner, dinv):
    panels = []
    uppers = []
    diags = []
    for group in range(N_LEAF):
        own_block = ainv_sep[group].astype(jnp.float32)
        sibling = ainv_sep[group ^ 1].astype(jnp.float32)
        colmask = jnp.repeat(owner[group], B)
        mixed = jnp.where(colmask[None, :] == 1, sibling, own_block)
        rowmask = jnp.repeat(jnp.repeat(block_mask[group].T, B, axis=0), B, axis=1)
        masked = jnp.where(rowmask == 1, l_panel[group], jnp.zeros((), jnp.bfloat16)).astype(jnp.float32)
        panel = (-jnp.dot(mixed, masked, precision=lax.Precision.HIGHEST)).astype(jnp.bfloat16)
        panels.append(panel)
        uppers.append(panel.T)
        panel_f = panel.astype(jnp.float32).reshape(SEP, NSUP, B)
        masked_f = masked.reshape(SEP, NSUP, B)
        update = jnp.einsum("ski,skc->kic", panel_f, masked_f, precision=lax.Precision.HIGHEST)
        diags.append(dinv[group] - update.reshape(NSUP * B, B))
    return jnp.stack(panels), jnp.stack(uppers), jnp.stack(diags)
```

```python
import functools

import jax
import jax.numpy as jnp
from jax import lax
from jax.experimental import pallas as pl
from jax.experimental.pallas import tpu as pltpu
from jax.sharding import PartitionSpec as P

MESH = pl.DeviceIdType.MESH
B = 512
SEP = 16384
ROWS = 256
NZ, NX, NY = 8, 4, 2
NGRID = NZ * NX * NY
LENGTH = {"z": NZ, "x": NX, "y": NY}

FIRST = (0, 80, 160)
COUNT = (80, 80, 96)
AXES = ("yxz", "yzx", "zxy")
OWN_ORDER = {"z": (2, 1, 0), "x": (0, 2, 1), "y": (0, 1, 2)}

EVENTS = (
    10, 201, 202, 27000, 21000, 10010, 20201, 20202, 17000, 11000, 20010, 7000, 1000, 10202,
    10201, 7010, 1010, 212, 211, 27010, 200, 21010, 7100, 7300, 1100, 1300, 27201, 27202,
    21201, 21202, 20310, 20110, 26000, 22000, 10212, 10211, 17010, 11010, 20200, 16000, 12000, 17201,
    17202, 27110, 27310, 6000, 2000, 11201, 11202, 6010, 2010, 210, 10200, 21110, 21310, 27200,
    7310, 7110, 1310, 1110, 21200, 26201, 26010, 1200, 7200, 26202, 22201, 22010, 6100, 2100,
    10210, 22202, 6300, 2300, 20210, 17212, 17211, 27210, 24001, 24002, 11211, 11212, 16010, 12010,
    16201, 16202, 21210, 14001, 14002, 12201, 12202, 4002, 4001, 26310, 26110, 17200, 26200, 4011,
    4012, 11200, 17210, 1210, 7210, 22200, 22310, 22110, 6310, 2310, 23201, 25201, 2110, 6110,
    23202, 25202, 11210, 23010, 25010, 2200, 6200, 12212, 12211, 4101, 4102, 26210, 16212, 16211,
    4301, 4302, 16200, 22210, 24000, 15201, 13201, 14011, 14012, 15202, 13202, 14000, 4000, 4010,
    23310, 23110, 23200, 12200, 16210, 6210, 2210, 25310, 25110, 25200, 12210, 4311, 4312, 4111,
    4112, 24201, 24202, 24010, 4202, 4201, 15200, 25210, 4100, 13200, 15211, 13211, 14010, 4212,
    4300, 23210, 4310, 13212, 15212, 14201, 4110, 4211, 14202, 24310, 24110, 4200, 24200, 13210,
    4210, 15210, 14211, 14212, 24210, 14200, 14210,
)
SITES = {
    36: (0, 1, 3, 28,),
    76: (4, 2, 29, 31,),
    83: (5, 7, 24, 8,),
    120: (30, 6, 9, 11,),
    134: (25, 27, 12, 20,),
    171: (26, 10, 16, 13,),
    181: (15, 21, 23, 14,),
    188: (22, 17, 19, 18,),
}


def decode(event):
    return event // 10000, event // 1000 % 10, event // 100 % 10, event // 10 % 10, event % 10


def last_axis(piece, offset):
    moved = [axis for axis in AXES[piece] if offset[axis]]
    return moved[-1] if moved else None


def side(piece, axis, source, core):
    z, x, y = source
    if piece == 0:
        bit = y + core if axis == "x" else x + y + core
    elif piece == 1:
        bit = y + core if axis == "z" else y + z + core
    else:
        bit = core if axis == "z" else z + core
    return 1 - 2 * (bit % 2)


def gather_schedule(me, core, start, take):
    z, x, y = me

    def moved(axis, step):
        if axis == "z":
            return (z + step + NZ) % NZ, x, y
        if axis == "x":
            return z, (x + step + NX) % NX, y
        return z, x, 1 - y

    def ways(axis):
        return (1,) if axis == "y" else (1, -1)

    for axis in "yzx":
        for piece in OWN_ORDER[axis]:
            for way in ways(axis):
                start(piece, me, moved(axis, way))
    for number, event in enumerate(EVENTS):
        piece, dz, dx, dy, kind = decode(event)
        offset = {"z": dz, "x": dx, "y": dy}
        axis = last_axis(piece, offset)
        source = [(z + dz) % NZ, (x + dx) % NX, (y + dy) % NY]
        onward = None
        if kind:
            way = side(piece, axis, source, core)
            half = LENGTH[axis] // 2
            place = half + way if kind == 1 else half - way
            if axis == "z":
                source[0] = (z + place) % NZ
            else:
                source[1] = (x + place) % NX
            if kind == 1:
                onward = way
        elif axis != "y":
            half = LENGTH[axis] // 2
            if offset[axis] < half - 1:
                onward = -1
            elif offset[axis] > half + 1:
                onward = 1
        take(piece, source)
        if onward is not None:
            start(piece, source, moved(axis, onward))
        for later in AXES[piece][AXES[piece].index(axis) + 1 :]:
            for way in ways(later):
                start(piece, source, moved(later, way))
        yield number


def index_of(place):
    return place[0] * (NX * NY) + place[1] * NY + place[2]


def kernel(
    a_hbm, l_hbm, mask_ref, owner_ref, dinv_ref,
    panel_ref, upper_ref, diag_ref,
    whole, own, other, total, turned, rows_in,
    load_sem, sib_send, sib_recv, send_sem, recv_sem, turn_send, turn_recv,
):
    leaf, here = lax.axis_index("leaf"), lax.axis_index("grid")
    core = leaf % 2
    sibling = leaf + 1 - 2 * core
    me = (here // (NX * NY), here // NY % NX, here % NY)

    mine = pltpu.make_async_copy(
        l_hbm.at[0], whole.at[pl.ds(pl.multiple_of(here * ROWS, ROWS), ROWS)], load_sem.at[0]
    )
    mine.start()
    chunk = SEP // 4
    loads = []
    for part in range(4):
        columns = pl.ds(part * chunk, chunk)
        loads.append(pltpu.make_async_copy(a_hbm.at[0, :, columns], own.at[:, columns], load_sem.at[1 + part]))
        loads[-1].start()

    barrier = pltpu.get_barrier_semaphore()
    pl.semaphore_signal(barrier, inc=1, device_id=(sibling, here), device_id_type=MESH)

    def greet(step, carry):
        pl.semaphore_signal(
            barrier, inc=1, device_id=(leaf, lax.rem(here + step, NGRID)), device_id_type=MESH
        )
        return carry

    lax.fori_loop(1, NGRID, greet, 0)
    pl.semaphore_wait(barrier, NGRID)
    mine.wait()

    sent = []

    def remote(piece, source, place, send):
        block = whole.at[
            pl.ds(pl.multiple_of(index_of(source) * ROWS + FIRST[piece], 16), COUNT[piece])
        ]
        return pltpu.make_async_remote_copy(
            src_ref=block,
            dst_ref=block,
            send_sem=send,
            recv_sem=recv_sem.at[piece, index_of(source)],
            device_id=(leaf, index_of(place)),
            device_id_type=MESH,
        )

    def start(piece, source, place):
        sent.append(remote(piece, source, place, send_sem.at[len(sent)]))
        sent[-1].start()

    def take(piece, source):
        remote(piece, source, me, send_sem.at[0]).wait_recv()

    def multiply(blocks):
        code = sum(block * 32**i for i, block in enumerate(blocks))

        def one(_, code):
            block = code % 32
            number = (me[0] + block // NX) % NZ * NX + (me[1] + block % NX) % NX
            columns = pl.ds(pl.multiple_of(number * B, B), B)
            swap = jnp.full((ROWS, B), owner_ref[number], jnp.int32) == 1
            keep = jnp.full((ROWS, B), mask_ref[number], jnp.int32) == 1
            mixed = jnp.where(swap, other[:, columns], own[:, columns])
            mixed = jnp.where(keep, mixed, jnp.zeros((), jnp.bfloat16))
            total[...] += jnp.dot(mixed, whole[columns, :], preferred_element_type=jnp.float32)
            return code // 32

        lax.fori_loop(0, len(blocks), one, jnp.int32(code))

    swaps = []
    for part in range(4):
        columns = pl.ds(part * chunk, chunk)
        swaps.append(
            pltpu.make_async_remote_copy(
                src_ref=a_hbm.at[0, :, columns],
                dst_ref=other.at[:, columns],
                send_sem=sib_send.at[part],
                recv_sem=sib_recv.at[part],
                device_id=(sibling, here),
                device_id_type=MESH,
            )
        )
    total[...] = jnp.zeros_like(total)
    ready = False
    for number in gather_schedule(me, core, start, take):
        if number == 4:
            for copy in swaps:
                copy.start()
        if number in SITES:
            if not ready:
                for copy in loads:
                    copy.wait()
                for copy in swaps:
                    copy.wait()
                ready = True
            multiply(SITES[number])

    panel = (-total[...]).astype(jnp.bfloat16)
    panel_ref[0] = panel
    turned[...] = panel.astype(jnp.float32).T.reshape(NGRID, B // NGRID, ROWS).astype(jnp.bfloat16)

    def column(place):
        return pl.ds(pl.multiple_of(place * ROWS, ROWS), ROWS)

    def turn(step, back):
        target = lax.rem(here + step, NGRID)
        return pltpu.make_async_remote_copy(
            src_ref=turned.at[target],
            dst_ref=rows_in.at[:, column(here if not back else lax.rem(here - step + NGRID, NGRID))],
            send_sem=turn_send.at[step],
            recv_sem=turn_recv.at[step],
            device_id=(leaf, target),
            device_id_type=MESH,
        )

    def send(step, carry):
        turn(step, False).start()
        return carry

    lax.fori_loop(1, NGRID, send, 0)
    rows_in[:, column(here)] = turned[here]
    for copy in sent:
        copy.wait_send()

    def arrive(step, carry):
        turn(step, True).wait_recv()
        return carry

    lax.fori_loop(1, NGRID, arrive, 0)
    upper_ref[0] = rows_in[...]

    def diagonal(number, total_rows):
        columns = pl.ds(pl.multiple_of(number * B, B), B)
        keep = jnp.full((B // NGRID, B), mask_ref[number], jnp.int32) == 1
        left = jnp.where(keep, rows_in[:, columns], jnp.zeros((), jnp.bfloat16))
        return total_rows + jnp.dot(left, whole[columns, :], preferred_element_type=jnp.float32)

    update = lax.fori_loop(
        0, SEP // B, diagonal, jnp.zeros((B // NGRID, B), jnp.float32), unroll=4
    )
    diag_ref[0] = dinv_ref[0] - update

    def leave(step, carry):
        turn(step, False).wait_send()
        return carry

    lax.fori_loop(1, NGRID, leave, 0)


def body(ainv_sep, l_panel, block_mask, owner, dinv):
    vmem = pl.BlockSpec(memory_space=pltpu.VMEM)
    smem = pl.BlockSpec(memory_space=pltpu.SMEM)
    hbm = pl.BlockSpec(memory_space=pl.ANY)
    dma = pltpu.SemaphoreType.DMA
    return pl.pallas_call(
        kernel,
        out_shape=(
            jax.ShapeDtypeStruct((1, ROWS, B), jnp.bfloat16),
            jax.ShapeDtypeStruct((1, B // NGRID, SEP), jnp.bfloat16),
            jax.ShapeDtypeStruct((1, B // NGRID, B), jnp.float32),
        ),
        in_specs=[hbm, hbm, smem, smem, vmem],
        out_specs=(vmem, vmem, vmem),
        scratch_shapes=[
            pltpu.VMEM((SEP, B), jnp.bfloat16),
            pltpu.VMEM((ROWS, SEP), jnp.bfloat16),
            pltpu.VMEM((ROWS, SEP), jnp.bfloat16),
            pltpu.VMEM((ROWS, B), jnp.float32),
            pltpu.VMEM((NGRID, B // NGRID, ROWS), jnp.bfloat16),
            pltpu.VMEM((B // NGRID, SEP), jnp.bfloat16),
            dma((5,)),
            dma((4,)),
            dma((4,)),
            dma((208,)),
            dma((3, NGRID)),
            dma((NGRID,)),
            dma((NGRID,)),
        ],
        compiler_params=pltpu.CompilerParams(
            collective_id=0, has_side_effects=True, vmem_limit_bytes=60 * 1024 * 1024
        ),
    )(ainv_sep, l_panel, block_mask.reshape(-1), owner.reshape(-1), dinv)


def solution(mesh):
    rows = P("leaf", "grid", None)
    return jax.shard_map(
        body,
        mesh=mesh,
        in_specs=(rows, rows, P("leaf", None, None), P("leaf", None), rows),
        out_specs=(rows, rows, rows),
        check_vma=False,
    )
```

```python
import functools

import jax
import jax.numpy as jnp
from jax import lax
from jax.experimental import pallas as pl
from jax.experimental.pallas import tpu as pltpu
from jax.sharding import PartitionSpec as P

MESH = pl.DeviceIdType.MESH
B = 512
SEP = 16384
ROWS = 256
NZ, NX, NY = 8, 4, 2
NGRID = NZ * NX * NY
LENGTH = {"z": NZ, "x": NX, "y": NY}
WAYS = (("z", 1), ("z", -1), ("x", 1), ("x", -1), ("y", 1))

FIRST = (0, 80, 160)
COUNT = (80, 80, 96)
AXES = ("yxz", "yzx", "zxy")
OWN_ORDER = {"z": (2, 1, 0), "x": (0, 2, 1), "y": (0, 1, 2)}

EVENTS = (
    10, 201, 202, 27000, 21000, 10010, 20201, 20202, 17000, 11000, 20010, 7000, 1000, 10202,
    10201, 7010, 1010, 212, 211, 27010, 200, 21010, 7100, 7300, 1100, 1300, 27201, 27202,
    21201, 21202, 20310, 20110, 26000, 22000, 10212, 10211, 17010, 11010, 20200, 16000, 12000, 17201,
    17202, 27110, 27310, 6000, 2000, 11201, 11202, 6010, 2010, 210, 10200, 21110, 21310, 27200,
    7310, 7110, 1310, 1110, 21200, 26201, 26010, 1200, 7200, 26202, 22201, 22010, 6100, 2100,
    10210, 22202, 6300, 2300, 20210, 17212, 17211, 27210, 24001, 24002, 11211, 11212, 16010, 12010,
    16201, 16202, 21210, 14001, 14002, 12201, 12202, 4002, 4001, 26310, 26110, 17200, 26200, 4011,
    4012, 11200, 17210, 1210, 7210, 22200, 22310, 22110, 6310, 2310, 23201, 25201, 2110, 6110,
    23202, 25202, 11210, 23010, 25010, 2200, 6200, 12212, 12211, 4101, 4102, 26210, 16212, 16211,
    4301, 4302, 16200, 22210, 24000, 15201, 13201, 14011, 14012, 15202, 13202, 14000, 4000, 4010,
    23310, 23110, 23200, 12200, 16210, 6210, 2210, 25310, 25110, 25200, 12210, 4311, 4312, 4111,
    4112, 24201, 24202, 24010, 4202, 4201, 15200, 25210, 4100, 13200, 15211, 13211, 14010, 4212,
    4300, 23210, 4310, 13212, 15212, 14201, 4110, 4211, 14202, 24310, 24110, 4200, 24200, 13210,
    4210, 15210, 14211, 14212, 24210, 14200, 14210,
)
SITES = {
    36: (0, 1, 3, 28,),
    76: (4, 2, 29, 31,),
    83: (5, 7, 24, 8,),
    120: (30, 6, 9, 11,),
    134: (25, 27, 12, 20,),
    171: (26, 10, 16, 13,),
    181: (15, 21, 23, 14,),
    188: (22, 17, 19, 18,),
}


def decode(event):
    return event // 10000, event // 1000 % 10, event // 100 % 10, event // 10 % 10, event % 10


def last_axis(piece, offset):
    moved = [axis for axis in AXES[piece] if offset[axis]]
    return moved[-1] if moved else None


def side(piece, axis, source, core):
    z, x, y = source
    if piece == 0:
        bit = y + core if axis == "x" else x + y + core
    elif piece == 1:
        bit = y + core if axis == "z" else y + z + core
    else:
        bit = core if axis == "z" else z + core
    return 1 - 2 * (bit % 2)


def moved(place, axis, step):
    z, x, y = place
    if axis == "z":
        return (z + step + NZ) % NZ, x, y
    if axis == "x":
        return z, (x + step + NX) % NX, y
    return z, x, 1 - y


def gather_schedule(me, core, start, take):
    z, x, y = me

    def ways(axis):
        return (1,) if axis == "y" else (1, -1)

    for axis in "yzx":
        for piece in OWN_ORDER[axis]:
            for way in ways(axis):
                start(piece, me, moved(me, axis, way))
    for number, event in enumerate(EVENTS):
        piece, dz, dx, dy, kind = decode(event)
        offset = {"z": dz, "x": dx, "y": dy}
        axis = last_axis(piece, offset)
        source = [(z + dz) % NZ, (x + dx) % NX, (y + dy) % NY]
        onward = None
        if kind:
            way = side(piece, axis, source, core)
            half = LENGTH[axis] // 2
            place = half + way if kind == 1 else half - way
            if axis == "z":
                source[0] = (z + place) % NZ
            else:
                source[1] = (x + place) % NX
            if kind == 1:
                onward = way
        elif axis != "y":
            half = LENGTH[axis] // 2
            if offset[axis] < half - 1:
                onward = -1
            elif offset[axis] > half + 1:
                onward = 1
        take(piece, source)
        if onward is not None:
            start(piece, source, moved(me, axis, onward))
        for later in AXES[piece][AXES[piece].index(axis) + 1 :]:
            for way in ways(later):
                start(piece, source, moved(me, later, way))
        yield number


def index_of(place):
    return place[0] * (NX * NY) + place[1] * NY + place[2]


def kernel(
    a_hbm, l_hbm, mask_ref, owner_ref, dinv_ref,
    panel_ref, upper_ref, diag_ref,
    whole, own, other, total, turned, rows_in,
    load_sem, sib_send, sib_recv, send_sem, recv_sem, turn_send, turn_recv,
):
    leaf, here = lax.axis_index("leaf"), lax.axis_index("grid")
    core = leaf % 2
    sibling = leaf + 1 - 2 * core
    me = (here // (NX * NY), here // NY % NX, here % NY)

    mine = pltpu.make_async_copy(
        l_hbm.at[0], whole.at[pl.ds(pl.multiple_of(here * ROWS, ROWS), ROWS)], load_sem.at[0]
    )
    mine.start()
    chunk = SEP // 4
    loads = []
    for part in range(4):
        columns = pl.ds(part * chunk, chunk)
        loads.append(pltpu.make_async_copy(a_hbm.at[0, :, columns], own.at[:, columns], load_sem.at[1 + part]))
        loads[-1].start()

    barrier = pltpu.get_barrier_semaphore()
    pl.semaphore_signal(barrier, inc=1, device_id=(sibling, here), device_id_type=MESH)
    for axis, way in WAYS:
        pl.semaphore_signal(
            barrier, inc=1, device_id=(leaf, index_of(moved(me, axis, way))), device_id_type=MESH
        )
    pl.semaphore_wait(barrier, 1 + len(WAYS))
    mine.wait()

    sent = []

    def remote(piece, source, place, send):
        block = whole.at[
            pl.ds(pl.multiple_of(index_of(source) * ROWS + FIRST[piece], 16), COUNT[piece])
        ]
        return pltpu.make_async_remote_copy(
            src_ref=block,
            dst_ref=block,
            send_sem=send,
            recv_sem=recv_sem.at[piece, index_of(source)],
            device_id=(leaf, index_of(place)),
            device_id_type=MESH,
        )

    def start(piece, source, place):
        sent.append(remote(piece, source, place, send_sem.at[len(sent)]))
        sent[-1].start()

    def take(piece, source):
        remote(piece, source, me, send_sem.at[0]).wait_recv()

    def multiply(blocks):
        code = sum(block * 32**i for i, block in enumerate(blocks))

        def one(_, code):
            block = code % 32
            number = (me[0] + block // NX) % NZ * NX + (me[1] + block % NX) % NX
            columns = pl.ds(pl.multiple_of(number * B, B), B)
            swap = jnp.full((ROWS, B), owner_ref[number], jnp.int32) == 1
            keep = jnp.full((ROWS, B), mask_ref[number], jnp.int32) == 1
            mixed = jnp.where(swap, other[:, columns], own[:, columns])
            mixed = jnp.where(keep, mixed, jnp.zeros((), jnp.bfloat16))
            total[...] += jnp.dot(mixed, whole[columns, :], preferred_element_type=jnp.float32)
            return code // 32

        lax.fori_loop(0, len(blocks), one, jnp.int32(code))

    swaps = []
    for part in range(4):
        columns = pl.ds(part * chunk, chunk)
        swaps.append(
            pltpu.make_async_remote_copy(
                src_ref=a_hbm.at[0, :, columns],
                dst_ref=other.at[:, columns],
                send_sem=sib_send.at[part],
                recv_sem=sib_recv.at[part],
                device_id=(sibling, here),
                device_id_type=MESH,
            )
        )
    total[...] = jnp.zeros_like(total)
    ready = False
    for number in gather_schedule(me, core, start, take):
        if number == 4:
            for copy in swaps:
                copy.start()
        if number in SITES:
            if not ready:
                for copy in loads:
                    copy.wait()
                for copy in swaps:
                    copy.wait()
                ready = True
            multiply(SITES[number])

    panel = (-total[...]).astype(jnp.bfloat16)
    panel_ref[0] = panel
    turned[...] = panel.astype(jnp.float32).T.reshape(NGRID, B // NGRID, ROWS).astype(jnp.bfloat16)

    def column(place):
        return pl.ds(pl.multiple_of(place * ROWS, ROWS), ROWS)

    def turn(step, back):
        target = lax.rem(here + step, NGRID)
        return pltpu.make_async_remote_copy(
            src_ref=turned.at[target],
            dst_ref=rows_in.at[:, column(here if not back else lax.rem(here - step + NGRID, NGRID))],
            send_sem=turn_send.at[step],
            recv_sem=turn_recv.at[step],
            device_id=(leaf, target),
            device_id_type=MESH,
        )

    def send(step, carry):
        turn(step, False).start()
        return carry

    lax.fori_loop(1, NGRID, send, 0)
    rows_in[:, column(here)] = turned[here]
    for copy in sent:
        copy.wait_send()

    def arrive(source):
        @pl.when(source != here)
        def _():
            turn(lax.rem(here - source + NGRID, NGRID), True).wait_recv()

    PLANE = NX * NY
    update = jnp.zeros((B // NGRID, B), jnp.float32)
    for dz in (0, 1, 7, 2, 6, 3, 5, 4):
        plane = (me[0] + dz) % NZ
        for i in range(PLANE):
            arrive(plane * PLANE + i)
        for i in range(PLANE // NY):
            number = plane * (PLANE // NY) + i
            columns = pl.ds(pl.multiple_of(number * B, B), B)
            keep = jnp.full((B // NGRID, B), mask_ref[number], jnp.int32) == 1
            left = jnp.where(keep, rows_in[:, columns], jnp.zeros((), jnp.bfloat16))
            update += jnp.dot(left, whole[columns, :], preferred_element_type=jnp.float32)
    upper_ref[0] = rows_in[...]
    diag_ref[0] = dinv_ref[0] - update

    def leave(step, carry):
        turn(step, False).wait_send()
        return carry

    lax.fori_loop(1, NGRID, leave, 0)


def body(ainv_sep, l_panel, block_mask, owner, dinv):
    vmem = pl.BlockSpec(memory_space=pltpu.VMEM)
    smem = pl.BlockSpec(memory_space=pltpu.SMEM)
    hbm = pl.BlockSpec(memory_space=pl.ANY)
    dma = pltpu.SemaphoreType.DMA
    return pl.pallas_call(
        kernel,
        out_shape=(
            pltpu.VMEM((1, ROWS, B), jnp.bfloat16),
            pltpu.VMEM((1, B // NGRID, SEP), jnp.bfloat16),
            pltpu.VMEM((1, B // NGRID, B), jnp.float32),
        ),
        in_specs=[hbm, hbm, smem, smem, vmem],
        out_specs=(vmem, vmem, vmem),
        scratch_shapes=[
            pltpu.VMEM((SEP, B), jnp.bfloat16),
            pltpu.VMEM((ROWS, SEP), jnp.bfloat16),
            pltpu.VMEM((ROWS, SEP), jnp.bfloat16),
            pltpu.VMEM((ROWS, B), jnp.float32),
            pltpu.VMEM((NGRID, B // NGRID, ROWS), jnp.bfloat16),
            pltpu.VMEM((B // NGRID, SEP), jnp.bfloat16),
            dma((5,)),
            dma((4,)),
            dma((4,)),
            dma((208,)),
            dma((3, NGRID)),
            dma((NGRID,)),
            dma((NGRID,)),
        ],
        compiler_params=pltpu.CompilerParams(
            collective_id=0, has_side_effects=True, vmem_limit_bytes=60 * 1024 * 1024
        ),
    )(ainv_sep, l_panel, block_mask.reshape(-1), owner.reshape(-1), dinv)


def solution(mesh):
    rows = P("leaf", "grid", None)
    return jax.shard_map(
        body,
        mesh=mesh,
        in_specs=(rows, rows, P("leaf", None, None), P("leaf", None), rows),
        out_specs=(rows, rows, rows),
        check_vma=False,
    )
```

```python
import functools

import jax
import jax.numpy as jnp
from jax import lax
from jax.experimental import pallas as pl
from jax.experimental.pallas import tpu as pltpu
from jax.sharding import PartitionSpec as P

MESH = pl.DeviceIdType.MESH
B = 512
SEP = 16384
ROWS = 256
NZ, NX, NY = 8, 4, 2
NGRID = NZ * NX * NY
WAYS = (("z", 1), ("z", -1), ("x", 1), ("x", -1), ("y", 1))

FIRST = (0, 80, 160)
COUNT = (80, 80, 96)
AXES = ("yxz", "yzx", "zxy")
PROGRAM = (
    22000, 32000, 42000, 52000, 12000, 10000, 21000, 31000, 40000, 50000, 11000, 20000, 30000, 41000, 51000,
    92001, 92500, 92100, 92030, 92010, 42100, 2500, 2100, 12100, 42500, 12500, 52500, 12030, 90001, 91500,
    91100, 90030, 90010, 40001, 50001, 1500, 1100, 10, 52100, 20001, 91030, 91010, 90100, 90500, 91001,
    31001, 21001, 12010, 2010, 92110, 92101, 92200, 92600, 2200, 2600, 42200, 20010, 42600, 20030, 92510,
    90031, 90011, 91600, 91200, 20011, 11, 92501, 12200, 41100, 92530, 1200, 20031, 91101, 91501, 1101,
    90020, 41500, 12600, 92031, 92130, 20020, 90101, 52200, 92020, 12510, 92011, 92300, 42300, 1501, 52600,
    92210, 2300, 90111, 90110, 41200, 92700, 90021, 20021, 12110, 92610, 41001, 42700, 90130, 30010, 41101,
    91110, 92201, 12130, 30011, 91300, 91201, 1201, 41300, 91510, 90131, 92310, 30030, 41600, 92601, 12530,
    30031, 90120, 30001, 92230, 2110, 52300, 41501, 30020, 91601, 92511, 92630, 100, 12020, 92400, 91210,
    90121, 42400, 2510, 91301, 92111, 91011, 12300, 92710, 1600, 90510, 91111, 91310, 92131, 90511, 30021,
    101, 2610, 12610, 91610, 90530, 111, 110, 90531, 41201, 90501, 92531, 2210, 12210, 91511, 51300,
    92120, 130, 131, 92330, 90520, 90200, 92021, 12700, 51500, 52700, 120, 41601, 92410, 92520, 500,
    1601, 91700, 51100, 92301, 12630, 41700, 2310, 1301, 121, 90521, 90201, 501, 92620, 92611, 12230,
    90211, 90210, 1010, 91211, 92220, 511, 530, 92211, 91330, 12120, 2710, 90230, 90231, 51001, 531,
    510, 51200, 91530, 92701, 91611, 92730, 90220, 12520, 52400, 51101, 520, 90600, 200, 91701, 91130,
    91710, 92631, 41301, 12310, 91401, 201, 51600, 92320, 90221, 521, 90601, 41701, 210, 92231, 51501,
    12710, 91020, 90611, 90630, 211, 230, 51201, 1510, 61310, 92121, 91031, 92720, 12400, 91230, 90631,
    90610, 231, 2410, 1110, 600, 92430, 92521, 12330, 90620, 91131, 220, 51601, 90300, 221, 91311,
    90301, 91630, 1210, 92311, 90621, 12620, 1011, 1300, 91711, 630, 90310, 91531, 1111, 41401, 92711,
    12220, 611, 90311, 610, 90330, 91231, 91410, 1610, 91520, 1310, 92401, 12730, 90331, 631, 601,
    1511, 92420, 91120, 51301, 90700, 90320, 91631, 620, 92331, 12410, 300, 51700, 1211, 90321, 61330,
    91220, 91021, 92621, 621, 12320, 91400, 51401, 1611, 90730, 301, 91121, 91411, 311, 92221, 1311,
    90711, 12720, 51701, 90710, 310, 91620, 91320, 331, 1410, 90701, 90731, 1710, 92731, 12430, 330,
    91521, 320, 91331, 1711, 1411, 90720, 321, 90400, 12420, 92411, 91730, 91221, 91430, 90721, 91431,
    92321, 91621, 90401, 90411, 91321, 91731, 92721, 90410, 90431, 91420, 91720, 90430, 92431, 90420, 91721,
    91421, 90421, 92421,
)
SITES = {
    159: (0, 4,),
    235: (28, 8,),
    250: (24, 1,),
    281: (3, 5,),
    290: (7, 29,),
    306: (31, 9,),
    315: (11, 25,),
    325: (27, 2,),
    339: (12, 20,),
    345: (6, 30,),
    361: (10, 26,),
    365: (16, 13,),
    369: (15, 21,),
    374: (23, 17,),
    377: (19, 14, 22, 18,),
}


def decode(item):
    return item // 10000, item // 1000 % 10, item // 100 % 10, item // 10 % 10, item % 10


def wrap(value, length):
    return value % length if isinstance(value, int) else lax.rem(value, length)


def side(piece, axis, source, core):
    z, x, y = source
    if piece == 0:
        bit = y + core if axis == "x" else x + y + core
    elif piece == 1:
        bit = y + core if axis == "z" else y + z + core
    else:
        bit = core if axis == "z" else z + core
    return 1 - 2 * wrap(bit, 2)


def locate(piece, kz, kx, dy, me, core):
    source = list(me)
    for axis in AXES[piece]:
        if axis == "y" and dy:
            source[2] = 1 - me[2]
        elif axis == "z" and kz:
            way = side(piece, axis, source, core)
            source[0] = wrap(me[0] + NZ + (-way * kz if kz <= 4 else way * (kz - 4)), NZ)
        elif axis == "x" and kx:
            way = side(piece, axis, source, core)
            source[1] = wrap(me[1] + NX + (-way * kx if kx <= 2 else way), NX)
    return tuple(source)


def moved(place, axis, step):
    z, x, y = place
    if axis == "z":
        return wrap(z + step + NZ, NZ), x, y
    if axis == "x":
        return z, wrap(x + step + NX, NX), y
    return z, x, 1 - y


def gather_schedule(me, core, start, take):
    for number, item in enumerate(PROGRAM):
        what, piece, kz, kx, dy = decode(item)
        source = locate(piece, kz, kx, dy, me, core)
        if what == 9:
            take(piece, source)
        else:
            short = what in (3, 5)
            if what:
                axis = {1: "y", 2: "z", 3: "z", 4: "x", 5: "x", 6: "z"}[what]
            else:
                places = {"z": kz, "x": kx, "y": dy}
                axis = [axis for axis in AXES[piece] if places[axis]][-1]
                short = axis == "z" and kz > 4
            way = side(piece, axis, source, core) if axis != "y" else 1
            start(piece, source, moved(me, axis, -way if short else way))
        yield number


def index_of(place):
    return place[0] * PLANE + place[1] * NY + place[2]


PLANE = NX * NY
SENT = 63
CHUNK = 1024
MIX_FROM = 110
MIX_STEP = 3


def kernel(
    a_hbm, l_hbm, mask_hbm, owner_hbm, dinv_hbm,
    panel_ref, upper_ref, diag_ref,
    whole, own, other, total, turned, mask_ref, owner_ref, dinv_ref,
    load_sem, send_sem, recv_sem, turn_send, turn_recv,
):
    leaf, here = lax.axis_index("leaf"), lax.axis_index("grid")
    core = lax.rem(leaf, 2)
    sibling = leaf + 1 - 2 * core
    me = (here // PLANE, lax.rem(here // NY, NX), lax.rem(here, NY))

    mine = pltpu.make_async_copy(
        l_hbm.at[0], whole.at[pl.ds(pl.multiple_of(here * ROWS, ROWS), ROWS)], load_sem.at[0]
    )
    mine.start()

    barrier = pltpu.get_barrier_semaphore()
    pl.semaphore_signal(barrier, inc=1, device_id=(sibling, here), device_id_type=MESH)
    for axis, way in WAYS:
        pl.semaphore_signal(
            barrier, inc=1, device_id=(leaf, index_of(moved(me, axis, way))), device_id_type=MESH
        )
    small = [
        pltpu.make_async_copy(mask_hbm, mask_ref, load_sem.at[1]),
        pltpu.make_async_copy(owner_hbm, owner_ref, load_sem.at[2]),
        pltpu.make_async_copy(dinv_hbm.at[0], dinv_ref, load_sem.at[3]),
    ]
    for copy in small:
        copy.start()
    pl.semaphore_wait(barrier, 1 + len(WAYS))
    mine.wait()

    def remote(piece, source, place):
        block = whole.at[
            pl.ds(pl.multiple_of(index_of(source) * ROWS + FIRST[piece], 16), COUNT[piece])
        ]
        return pltpu.make_async_remote_copy(
            src_ref=block,
            dst_ref=block,
            send_sem=send_sem.at[piece],
            recv_sem=recv_sem.at[piece, index_of(source)],
            device_id=(leaf, index_of(place)),
            device_id_type=MESH,
        )

    def start(piece, source, place):
        remote(piece, source, place).start()

    def take(piece, source):
        remote(piece, source, me).wait_recv()

    def multiply(blocks):
        product = None
        for block in blocks:
            number = moved(me, "z", block // NX)[0] * NX + moved(me, "x", block % NX)[1]
            columns = pl.ds(pl.multiple_of(number * B, B), B)
            part = jnp.dot(own[:, columns], whole[columns, :], preferred_element_type=jnp.float32)
            product = part if product is None else product + part
        total[...] += product

    def mix(first, count):
        def one(number, carry):
            columns = pl.ds(pl.multiple_of(number * B, B), B)
            swap = jnp.full((ROWS, B), owner_ref[number], jnp.int32) == 1
            keep = jnp.full((ROWS, B), mask_ref[number], jnp.int32) == 1
            mixed = jnp.where(swap, other[:, columns], own[:, columns])
            own[:, columns] = jnp.where(keep, mixed, jnp.zeros((), jnp.bfloat16))
            return carry

        lax.fori_loop(first, first + count, one, 0)

    def load(columns):
        return pltpu.make_async_copy(a_hbm.at[0, :, columns], own.at[:, columns], load_sem.at[4])

    def swap(columns):
        return pltpu.make_async_remote_copy(
            src_ref=a_hbm.at[0, :, columns],
            dst_ref=other.at[:, columns],
            send_sem=load_sem.at[5],
            recv_sem=load_sem.at[6],
            device_id=(sibling, here),
            device_id_type=MESH,
        )

    total[...] = jnp.zeros_like(total)
    issued, mixed = 0, 0
    for number in gather_schedule(me, core, start, take):
        if number % 4 == 3 and issued < SEP // CHUNK:
            columns = pl.ds(issued * CHUNK, CHUNK)
            load(columns).start()
            swap(columns).start()
            issued += 1
        if number == MIX_FROM:
            everything = pl.ds(0, SEP)
            for copy in small[:2] + [load(everything), swap(everything)]:
                copy.wait()
        if number >= MIX_FROM and (number - MIX_FROM) % MIX_STEP == 0 and mixed < SEP // B:
            mix(mixed, 2)
            mixed += 2
        if number in SITES:
            multiply(SITES[number])

    panel = (-total[...]).astype(jnp.bfloat16)
    turned[...] = panel.astype(jnp.float32).T.reshape(NGRID, B // NGRID, ROWS).astype(jnp.bfloat16)
    panel_ref[0] = panel

    rows_in = upper_ref.at[0]

    def column(place):
        return pl.ds(pl.multiple_of(place * ROWS, ROWS), ROWS)

    def turn(block, source, target):
        return pltpu.make_async_remote_copy(
            src_ref=block,
            dst_ref=rows_in.at[:, column(source)],
            send_sem=turn_send.at[0],
            recv_sem=turn_recv.at[source // PLANE],
            device_id=(leaf, target),
            device_id_type=MESH,
        )

    for dz in (4, 3, 5, 2, 6, 1, 7, 0):
        plane = moved(me, "z", dz)[0] * PLANE
        for i in range(PLANE):
            if dz == 0 and i == 0:
                continue
            target = plane + (here + i) % PLANE
            turn(turned.at[target], here, target).start()
    rows_in[:, column(here)] = turned[here]
    for piece in range(3):
        rows = whole.at[pl.ds(0, SENT * COUNT[piece])]
        pltpu.make_async_remote_copy(
            src_ref=rows, dst_ref=rows, send_sem=send_sem.at[piece], recv_sem=recv_sem.at[piece, 0],
            device_id=(sibling, here), device_id_type=MESH,
        ).wait_send()

    update = jnp.zeros((B // NGRID, B), jnp.float32)
    for dz in (0, 7, 1, 6, 2, 5, 3, 4):
        plane = moved(me, "z", dz)[0]
        count = PLANE if dz else PLANE - 1
        arrived = rows_in.at[:, pl.ds(0, count * ROWS)]
        pltpu.make_async_remote_copy(
            src_ref=arrived, dst_ref=arrived, send_sem=turn_send.at[0], recv_sem=turn_recv.at[plane],
            device_id=(sibling, here), device_id_type=MESH,
        ).wait_recv()
        for i in range(PLANE // NY):
            number = plane * (PLANE // NY) + i
            columns = pl.ds(pl.multiple_of(number * B, B), B)
            keep = jnp.full((B // NGRID, B), mask_ref[number], jnp.int32) == 1
            left = jnp.where(keep, rows_in[:, columns], jnp.zeros((), jnp.bfloat16))
            update += jnp.dot(left, whole[columns, :], preferred_element_type=jnp.float32)
    small[2].wait()
    diag_ref[0] = dinv_ref[...] - update

    direct = turned.at[pl.ds(0, NGRID - 1)]
    pltpu.make_async_remote_copy(
        src_ref=direct, dst_ref=direct, send_sem=turn_send.at[0], recv_sem=turn_recv.at[0],
        device_id=(sibling, here), device_id_type=MESH,
    ).wait_send()


def put_out(panel_ref, upper_ref, diag_ref, panel_out, upper_out, diag_out, sem):
    pairs = ((panel_ref, panel_out), (upper_ref, upper_out), (diag_ref, diag_out))
    copies = [pltpu.make_async_copy(a, b, sem.at[i]) for i, (a, b) in enumerate(pairs)]
    for copy in copies:
        copy.start()
    for copy in copies:
        copy.wait()


def body(ainv_sep, l_panel, block_mask, owner, dinv):
    vmem = pl.BlockSpec(memory_space=pltpu.VMEM)
    hbm = pl.BlockSpec(memory_space=pl.ANY)
    dma = pltpu.SemaphoreType.DMA
    shapes = (
        ((1, ROWS, B), jnp.bfloat16),
        ((1, B // NGRID, SEP), jnp.bfloat16),
        ((1, B // NGRID, B), jnp.float32),
    )
    results = pl.pallas_call(
        kernel,
        out_shape=tuple(pltpu.VMEM(*shape) for shape in shapes),
        in_specs=[hbm] * 5,
        out_specs=(vmem, vmem, vmem),
        scratch_shapes=[
            pltpu.VMEM((SEP, B), jnp.bfloat16),
            pltpu.VMEM((ROWS, SEP), jnp.bfloat16),
            pltpu.VMEM((ROWS, SEP), jnp.bfloat16),
            pltpu.VMEM((ROWS, B), jnp.float32),
            pltpu.VMEM((NGRID, B // NGRID, ROWS), jnp.bfloat16),
            pltpu.SMEM((SEP // B,), jnp.int32),
            pltpu.SMEM((SEP // B,), jnp.int32),
            pltpu.VMEM((B // NGRID, B), jnp.float32),
            dma((7,)),
            dma((3,)),
            dma((3, NGRID)),
            dma((1,)),
            dma((NZ,)),
        ],
        compiler_params=pltpu.CompilerParams(
            collective_id=0, has_side_effects=True, vmem_limit_bytes=60 * 1024 * 1024
        ),
    )(ainv_sep, l_panel, block_mask.reshape(-1), owner.reshape(-1), dinv)
    results = [pltpu.with_memory_space_constraint(result, pltpu.VMEM) for result in results]
    return pl.pallas_call(
        put_out,
        out_shape=tuple(jax.ShapeDtypeStruct(*shape) for shape in shapes),
        in_specs=[vmem] * 3,
        out_specs=(hbm, hbm, hbm),
        scratch_shapes=[dma((3,))],
    )(*results)


def solution(mesh):
    rows = P("leaf", "grid", None)
    return jax.shard_map(
        body,
        mesh=mesh,
        in_specs=(rows, rows, P("leaf", None, None), P("leaf", None), rows),
        out_specs=(rows, rows, rows),
        check_vma=False,
    )
```

```python
import functools

import jax
import jax.numpy as jnp
from jax import lax
from jax.experimental import pallas as pl
from jax.experimental.pallas import tpu as pltpu
from jax.sharding import PartitionSpec as P

MESH = pl.DeviceIdType.MESH
B = 512
SEP = 16384
ROWS = 256
NZ, NX, NY = 8, 4, 2
NGRID = NZ * NX * NY
WAYS = (("z", 1), ("z", -1), ("x", 1), ("x", -1), ("y", 1))

FIRST = (0, 80, 160)
COUNT = (80, 80, 96)
AXES = ("yxz", "yzx", "zxy")
PROGRAM = (
    22000, 32000, 42000, 52000, 12000, 10000, 21000, 31000, 40000, 50000, 11000, 20000, 30000, 41000, 51000,
    92001, 92500, 92100, 92030, 92010, 42100, 2500, 2100, 12100, 42500, 12500, 52500, 12030, 90001, 91500,
    91100, 90030, 90010, 40001, 50001, 1500, 1100, 10, 52100, 20001, 91030, 91010, 90100, 90500, 91001,
    31001, 21001, 12010, 2010, 92110, 92101, 92200, 92600, 2200, 2600, 42200, 20010, 42600, 20030, 92510,
    90031, 90011, 91600, 91200, 20011, 11, 92501, 12200, 41100, 92530, 1200, 20031, 91101, 91501, 1101,
    90020, 41500, 12600, 92031, 92130, 20020, 90101, 52200, 92020, 12510, 92011, 92300, 42300, 1501, 52600,
    92210, 2300, 90111, 90110, 41200, 92700, 90021, 20021, 12110, 92610, 41001, 42700, 90130, 30010, 41101,
    91110, 92201, 12130, 30011, 91300, 91201, 1201, 41300, 91510, 90131, 92310, 30030, 41600, 92601, 12530,
    30031, 90120, 30001, 92230, 2110, 52300, 41501, 30020, 91601, 92511, 92630, 100, 12020, 92400, 91210,
    90121, 42400, 2510, 91301, 92111, 91011, 12300, 92710, 1600, 90510, 91111, 91310, 92131, 90511, 30021,
    101, 2610, 12610, 91610, 90530, 111, 110, 90531, 41201, 90501, 92531, 2210, 12210, 91511, 51300,
    92120, 130, 131, 92330, 90520, 90200, 92021, 12700, 51500, 52700, 120, 41601, 92410, 92520, 500,
    1601, 91700, 51100, 92301, 12630, 41700, 2310, 1301, 121, 90521, 90201, 501, 92620, 92611, 12230,
    90211, 90210, 1010, 91211, 92220, 511, 530, 92211, 91330, 12120, 2710, 90230, 90231, 51001, 531,
    510, 51200, 91530, 92701, 91611, 92730, 90220, 12520, 52400, 51101, 520, 90600, 200, 91701, 91130,
    91710, 92631, 41301, 12310, 91401, 201, 51600, 92320, 90221, 521, 90601, 41701, 210, 92231, 51501,
    12710, 91020, 90611, 90630, 211, 230, 51201, 1510, 61310, 92121, 91031, 92720, 12400, 91230, 90631,
    90610, 231, 2410, 1110, 600, 92430, 92521, 12330, 90620, 91131, 220, 51601, 90300, 221, 91311,
    90301, 91630, 1210, 92311, 90621, 12620, 1011, 1300, 91711, 630, 90310, 91531, 1111, 41401, 92711,
    12220, 611, 90311, 610, 90330, 91231, 91410, 1610, 91520, 1310, 92401, 12730, 90331, 631, 601,
    1511, 92420, 91120, 51301, 90700, 90320, 91631, 620, 92331, 12410, 300, 51700, 1211, 90321, 61330,
    91220, 91021, 92621, 621, 12320, 91400, 51401, 1611, 90730, 301, 91121, 91411, 311, 92221, 1311,
    90711, 12720, 51701, 90710, 310, 91620, 91320, 331, 1410, 90701, 90731, 1710, 92731, 12430, 330,
    91521, 320, 91331, 1711, 1411, 90720, 321, 90400, 12420, 92411, 91730, 91221, 91430, 90721, 91431,
    92321, 91621, 90401, 90411, 91321, 91731, 92721, 90410, 90431, 91420, 91720, 90430, 92431, 90420, 91721,
    91421, 90421, 92421,
)
SITES = {
    159: (0, 4,),
    235: (28, 24,),
    250: (8, 1,),
    290: (3, 29, 5, 7,),
    316: (31, 2, 27, 11, 25, 9,),
    342: (20, 12,),
    352: (30, 6,),
    361: (10, 26,),
    365: (21, 16, 13, 23,),
    373: (15, 19,),
    377: (17, 22, 14, 18,),
}


def decode(item):
    return item // 10000, item // 1000 % 10, item // 100 % 10, item // 10 % 10, item % 10


def wrap(value, length):
    return value % length if isinstance(value, int) else lax.rem(value, length)


def side(piece, axis, source, core):
    z, x, y = source
    if piece == 0:
        bit = y + core if axis == "x" else x + y + core
    elif piece == 1:
        bit = y + core if axis == "z" else y + z + core
    else:
        bit = core if axis == "z" else z + core
    return 1 - 2 * wrap(bit, 2)


def locate(piece, kz, kx, dy, me, core):
    source = list(me)
    for axis in AXES[piece]:
        if axis == "y" and dy:
            source[2] = 1 - me[2]
        elif axis == "z" and kz:
            way = side(piece, axis, source, core)
            source[0] = wrap(me[0] + NZ + (-way * kz if kz <= 4 else way * (kz - 4)), NZ)
        elif axis == "x" and kx:
            way = side(piece, axis, source, core)
            source[1] = wrap(me[1] + NX + (-way * kx if kx <= 2 else way), NX)
    return tuple(source)


def moved(place, axis, step):
    z, x, y = place
    if axis == "z":
        return wrap(z + step + NZ, NZ), x, y
    if axis == "x":
        return z, wrap(x + step + NX, NX), y
    return z, x, 1 - y


def gather_schedule(me, core, start, take):
    for number, item in enumerate(PROGRAM):
        what, piece, kz, kx, dy = decode(item)
        if what == 9:
            if number in ENDS:
                take(ENDS[number])
        else:
            source = locate(piece, kz, kx, dy, me, core)
            short = what in (3, 5)
            if what:
                axis = {1: "y", 2: "z", 3: "z", 4: "x", 5: "x", 6: "z"}[what]
            else:
                places = {"z": kz, "x": kx, "y": dy}
                axis = [axis for axis in AXES[piece] if places[axis]][-1]
                short = axis == "z" and kz > 4
            way = side(piece, axis, source, core) if axis != "y" else 1
            start(piece, source, moved(me, axis, -way if short else way), SLOTS[receiver(what, piece, kz, kx, dy)])
        yield number


def receiver(what, piece, kz, kx, dy):
    if what == 0:
        if [axis for axis in AXES[piece] if {"z": kz, "x": kx, "y": dy}[axis]][-1] == "z":
            return piece, kz + 1, kx, dy
        return piece, kz, kx + 1, dy
    if what == 1:
        return piece, kz, kx, 1
    if what in (2, 3):
        return piece, 1 if what == 2 else 5, kx, dy
    if what in (4, 5):
        return piece, kz, 1 if what == 4 else 3, dy
    return piece, 4, kx, dy


def receive_slots(together):
    keys = {decode(item)[1:] for item in PROGRAM if item // 10000 != 9}
    slots, ends, last = {}, {}, []
    count = 0
    for number, item in enumerate(PROGRAM):
        what, *key = decode(item)
        key = tuple(key)
        if what != 9:
            continue
        if key in keys:
            slots[key] = count
            ends[number] = [key]
            count += 1
            continue
        last.append((number, key))
        if len(last) == together:
            ends[number] = [key for _, key in last]
            for _, key in last:
                slots[key] = count
            count += 1
            last = []
    if last:
        ends[last[-1][0]] = [key for _, key in last]
        for _, key in last:
            slots[key] = count
        count += 1
    return slots, ends, count


def index_of(place):
    return place[0] * PLANE + place[1] * NY + place[2]


PLANE = NX * NY
SENT = 63
CHUNK = 1024
TOGETHER = 4
SLOTS, ENDS, SLOT_COUNT = receive_slots(TOGETHER)
MIX_FROM = 110
MIX_STEP = 3


def kernel(
    a_hbm, l_hbm, mask_hbm, owner_hbm, dinv_hbm,
    panel_ref, upper_ref, diag_ref,
    whole, own, other, total, turned, mask_ref, owner_ref, dinv_ref,
    load_sem, send_sem, recv_sem, turn_send, turn_recv,
):
    leaf, here = lax.axis_index("leaf"), lax.axis_index("grid")
    core = lax.rem(leaf, 2)
    sibling = leaf + 1 - 2 * core
    me = (here // PLANE, lax.rem(here // NY, NX), lax.rem(here, NY))

    mine = pltpu.make_async_copy(
        l_hbm.at[0], whole.at[pl.ds(pl.multiple_of(here * ROWS, ROWS), ROWS)], load_sem.at[0]
    )
    mine.start()

    barrier = pltpu.get_barrier_semaphore()
    pl.semaphore_signal(barrier, inc=1, device_id=(sibling, here), device_id_type=MESH)
    for axis, way in WAYS:
        pl.semaphore_signal(
            barrier, inc=1, device_id=(leaf, index_of(moved(me, axis, way))), device_id_type=MESH
        )
    small = [
        pltpu.make_async_copy(mask_hbm, mask_ref, load_sem.at[1]),
        pltpu.make_async_copy(owner_hbm, owner_ref, load_sem.at[2]),
        pltpu.make_async_copy(dinv_hbm.at[0], dinv_ref, load_sem.at[3]),
    ]
    for copy in small:
        copy.start()
    pl.semaphore_wait(barrier, 1 + len(WAYS))
    mine.wait()

    def start(piece, source, place, slot):
        block = whole.at[
            pl.ds(pl.multiple_of(index_of(source) * ROWS + FIRST[piece], 16), COUNT[piece])
        ]
        pltpu.make_async_remote_copy(
            src_ref=block,
            dst_ref=block,
            send_sem=send_sem.at[piece],
            recv_sem=recv_sem.at[slot],
            device_id=(leaf, index_of(place)),
            device_id_type=MESH,
        ).start()

    def take(places):
        rows = whole.at[pl.ds(0, sum(COUNT[place[0]] for place in places))]
        pltpu.make_async_remote_copy(
            src_ref=rows, dst_ref=rows, send_sem=send_sem.at[0], recv_sem=recv_sem.at[SLOTS[places[0]]],
            device_id=(sibling, here), device_id_type=MESH,
        ).wait_recv()

    def multiply(blocks):
        product = None
        for block in blocks:
            number = moved(me, "z", block // NX)[0] * NX + moved(me, "x", block % NX)[1]
            columns = pl.ds(pl.multiple_of(number * B, B), B)
            part = jnp.dot(own[:, columns], whole[columns, :], preferred_element_type=jnp.float32)
            product = part if product is None else product + part
        total[...] += product

    def mix(first, count):
        def one(number, carry):
            columns = pl.ds(pl.multiple_of(number * B, B), B)
            swap = jnp.full((ROWS, B), owner_ref[number], jnp.int32) == 1
            keep = jnp.full((ROWS, B), mask_ref[number], jnp.int32) == 1
            mixed = jnp.where(swap, other[:, columns], own[:, columns])
            own[:, columns] = jnp.where(keep, mixed, jnp.zeros((), jnp.bfloat16))
            return carry

        lax.fori_loop(first, first + count, one, 0)

    def load(columns):
        return pltpu.make_async_copy(a_hbm.at[0, :, columns], own.at[:, columns], load_sem.at[4])

    def swap(columns):
        return pltpu.make_async_remote_copy(
            src_ref=a_hbm.at[0, :, columns],
            dst_ref=other.at[:, columns],
            send_sem=load_sem.at[5],
            recv_sem=load_sem.at[6],
            device_id=(sibling, here),
            device_id_type=MESH,
        )

    total[...] = jnp.zeros_like(total)
    issued, mixed = 0, 0
    for number in gather_schedule(me, core, start, take):
        if number % 4 == 3 and issued < SEP // CHUNK:
            columns = pl.ds(issued * CHUNK, CHUNK)
            load(columns).start()
            swap(columns).start()
            issued += 1
        if number == MIX_FROM:
            everything = pl.ds(0, SEP)
            for copy in small[:2] + [load(everything), swap(everything)]:
                copy.wait()
        if number >= MIX_FROM and (number - MIX_FROM) % MIX_STEP == 0 and mixed < SEP // B:
            mix(mixed, 2)
            mixed += 2
        if number in SITES:
            multiply(SITES[number])

    panel = (-total[...]).astype(jnp.bfloat16)
    turned[...] = panel.astype(jnp.float32).T.reshape(NGRID, B // NGRID, ROWS).astype(jnp.bfloat16)
    panel_ref[0] = panel

    rows_in = upper_ref.at[0]

    def column(place):
        return pl.ds(pl.multiple_of(place * ROWS, ROWS), ROWS)

    def turn(block, source, target):
        return pltpu.make_async_remote_copy(
            src_ref=block,
            dst_ref=rows_in.at[:, column(source)],
            send_sem=turn_send.at[0],
            recv_sem=turn_recv.at[source // PLANE],
            device_id=(leaf, target),
            device_id_type=MESH,
        )

    for dz in (4, 3, 5, 1, 7, 2, 6, 0):
        plane = moved(me, "z", dz)[0] * PLANE
        for i in range(PLANE):
            if dz == 0 and i == 0:
                continue
            target = plane + (here + i) % PLANE
            turn(turned.at[target], here, target).start()
    rows_in[:, column(here)] = turned[here]
    for piece in range(3):
        rows = whole.at[pl.ds(0, SENT * COUNT[piece])]
        pltpu.make_async_remote_copy(
            src_ref=rows, dst_ref=rows, send_sem=send_sem.at[piece], recv_sem=recv_sem.at[0],
            device_id=(sibling, here), device_id_type=MESH,
        ).wait_send()

    update = jnp.zeros((B // NGRID, B), jnp.float32)
    for dz in (4, 0, 3, 5, 1, 7, 6, 2):
        plane = moved(me, "z", dz)[0]
        count = PLANE if dz else PLANE - 1
        arrived = rows_in.at[:, pl.ds(0, count * ROWS)]
        pltpu.make_async_remote_copy(
            src_ref=arrived, dst_ref=arrived, send_sem=turn_send.at[0], recv_sem=turn_recv.at[plane],
            device_id=(sibling, here), device_id_type=MESH,
        ).wait_recv()
        for i in range(PLANE // NY):
            number = plane * (PLANE // NY) + i
            columns = pl.ds(pl.multiple_of(number * B, B), B)
            keep = jnp.full((B // NGRID, B), mask_ref[number], jnp.int32) == 1
            left = jnp.where(keep, rows_in[:, columns], jnp.zeros((), jnp.bfloat16))
            update += jnp.dot(left, whole[columns, :], preferred_element_type=jnp.float32)
    small[2].wait()
    diag_ref[0] = dinv_ref[...] - update

    direct = turned.at[pl.ds(0, NGRID - 1)]
    pltpu.make_async_remote_copy(
        src_ref=direct, dst_ref=direct, send_sem=turn_send.at[0], recv_sem=turn_recv.at[0],
        device_id=(sibling, here), device_id_type=MESH,
    ).wait_send()


def put_out(panel_ref, upper_ref, diag_ref, panel_out, upper_out, diag_out, sem):
    pairs = ((panel_ref, panel_out), (upper_ref, upper_out), (diag_ref, diag_out))
    copies = [pltpu.make_async_copy(a, b, sem.at[i]) for i, (a, b) in enumerate(pairs)]
    for copy in copies:
        copy.start()
    for copy in copies:
        copy.wait()


def body(ainv_sep, l_panel, block_mask, owner, dinv):
    vmem = pl.BlockSpec(memory_space=pltpu.VMEM)
    hbm = pl.BlockSpec(memory_space=pl.ANY)
    dma = pltpu.SemaphoreType.DMA
    shapes = (
        ((1, ROWS, B), jnp.bfloat16),
        ((1, B // NGRID, SEP), jnp.bfloat16),
        ((1, B // NGRID, B), jnp.float32),
    )
    results = pl.pallas_call(
        kernel,
        out_shape=tuple(pltpu.VMEM(*shape) for shape in shapes),
        in_specs=[hbm] * 5,
        out_specs=(vmem, vmem, vmem),
        scratch_shapes=[
            pltpu.VMEM((SEP, B), jnp.bfloat16),
            pltpu.VMEM((ROWS, SEP), jnp.bfloat16),
            pltpu.VMEM((ROWS, SEP), jnp.bfloat16),
            pltpu.VMEM((ROWS, B), jnp.float32),
            pltpu.VMEM((NGRID, B // NGRID, ROWS), jnp.bfloat16),
            pltpu.SMEM((SEP // B,), jnp.int32),
            pltpu.SMEM((SEP // B,), jnp.int32),
            pltpu.VMEM((B // NGRID, B), jnp.float32),
            dma((7,)),
            dma((3,)),
            dma((SLOT_COUNT,)),
            dma((1,)),
            dma((NZ,)),
        ],
        compiler_params=pltpu.CompilerParams(
            collective_id=0, has_side_effects=True, vmem_limit_bytes=60 * 1024 * 1024
        ),
    )(ainv_sep, l_panel, block_mask.reshape(-1), owner.reshape(-1), dinv)
    results = [pltpu.with_memory_space_constraint(result, pltpu.VMEM) for result in results]
    return pl.pallas_call(
        put_out,
        out_shape=tuple(jax.ShapeDtypeStruct(*shape) for shape in shapes),
        in_specs=[vmem] * 3,
        out_specs=(hbm, hbm, hbm),
        scratch_shapes=[dma((3,))],
    )(*results)


def solution(mesh):
    rows = P("leaf", "grid", None)
    return jax.shard_map(
        body,
        mesh=mesh,
        in_specs=(rows, rows, P("leaf", None, None), P("leaf", None), rows),
        out_specs=(rows, rows, rows),
        check_vma=False,
    )
```

```python
import functools

import jax
import jax.numpy as jnp
from jax import lax
from jax.experimental import pallas as pl
from jax.experimental.pallas import tpu as pltpu
from jax.sharding import PartitionSpec as P

MESH = pl.DeviceIdType.MESH
B = 512
SEP = 16384
ROWS = 256
NZ, NX, NY = 8, 4, 2
NGRID = NZ * NX * NY
WAYS = (("z", 1), ("z", -1), ("x", 1), ("x", -1), ("y", 1))

FIRST = (0, 80, 160)
COUNT = (80, 80, 96)
AXES = ("yxz", "yzx", "zxy")
PROGRAM = (
    22000, 32000, 42000, 52000, 12000, 10000, 21000, 31000, 50000, 40000, 11000, 20000, 30000, 41000, 51000,
    92001, 92500, 92100, 92030, 92010, 2500, 2100, 42100, 12100, 52500, 52100, 12500, 42500, 12030, 2010,
    12010, 90001, 91500, 91100, 90010, 90030, 1100, 20001, 1500, 20010, 50001, 40001, 20030, 10, 91001,
    90500, 90100, 91030, 91010, 31001, 21001, 92200, 92600, 52600, 2200, 2600, 12200, 42200, 52200, 12600,
    42600, 92530, 92101, 92110, 2110, 91200, 92501, 92130, 92510, 12510, 2510, 12110, 90101, 30010, 41100,
    1200, 91600, 92020, 92031, 90110, 12130, 30030, 90031, 20031, 90011, 20011, 11, 41500, 91501, 91101,
    1101, 90130, 30011, 30001, 92011, 12530, 90020, 20020, 92630, 92700, 42700, 92300, 42300, 52300, 2300,
    30031, 92201, 1501, 90111, 12020, 41001, 92210, 92230, 2210, 30020, 41200, 100, 92601, 12300, 90021,
    20021, 92610, 2610, 101, 91201, 41101, 52700, 90131, 92120, 92511, 41501, 130, 12610, 90120, 30021,
    1201, 92520, 41600, 110, 92111, 90510, 12210, 111, 91110, 90121, 91300, 41300, 92310, 92330, 90530,
    2310, 92131, 91510, 1600, 92400, 12700, 51100, 42400, 131, 90511, 90501, 41201, 500, 92531, 51500,
    12630, 92710, 120, 92620, 90531, 2710, 121, 91601, 91011, 92021, 530, 12230, 90520, 91210, 92220,
    90200, 41601, 501, 1010, 91111, 511, 92301, 90201, 12120, 92730, 52400, 1601, 51200, 510, 51001,
    91511, 531, 90230, 92611, 90521, 91301, 51101, 12520, 91310, 91610, 520, 90210, 200, 90211, 92211,
    51300, 12310, 201, 521, 91700, 41700, 51501, 92320, 41301, 91130, 92701, 92410, 90231, 12710, 230,
    91211, 90600, 2410, 51600, 91530, 90220, 211, 92631, 1301, 210, 12400, 90221, 51201, 92720, 90630,
    231, 1110, 92231, 91611, 12330, 600, 90601, 91020, 220, 90611, 1510, 51601, 91701, 41701, 91230,
    92121, 92430, 12620, 221, 90610, 91031, 601, 90631, 1011, 1210, 91131, 92521, 12220, 630, 90620,
    611, 1310, 90300, 1111, 91710, 91330, 61310, 92311, 610, 90301, 12730, 51301, 90621, 1511, 91531,
    91311, 631, 90330, 92711, 1300, 12410, 1610, 91630, 92420, 620, 90311, 91401, 41401, 300, 90310,
    91231, 1211, 92401, 51700, 12320, 301, 90331, 621, 91120, 91711, 51701, 1311, 92331, 90700, 12720,
    330, 90320, 311, 91520, 91631, 1611, 51401, 90321, 92621, 310, 90701, 12430, 91021, 91220, 331,
    1710, 1711, 90730, 61330, 92221, 321, 320, 90711, 12420, 91320, 91121, 91410, 1410, 90710, 91331,
    92731, 91521, 90731, 91400, 91411, 1411, 91620, 92411, 90720, 90400, 91221, 91730, 92321, 90401, 90721,
    91731, 91321, 90430, 90411, 92721, 91621, 91431, 90410, 90431, 92431, 91720, 91721, 91430, 90421, 90420,
    91421, 91420, 92421,
)
SITES = {
    160: (0, 4,),
    246: (28, 24,),
    277: (8, 1,),
    300: (3, 7, 29, 31,),
    325: (5, 9, 12, 20, 27, 25,),
    334: (11, 2,),
    347: (30, 6,),
    361: (21, 23, 16, 13,),
    365: (15, 10,),
    373: (26, 22, 19, 14,),
    377: (17, 18,),
}


def decode(item):
    return item // 10000, item // 1000 % 10, item // 100 % 10, item // 10 % 10, item % 10


def wrap(value, length):
    return value % length if isinstance(value, int) else lax.rem(value, length)


def side(piece, axis, source, core):
    z, x, y = source
    if piece == 0:
        bit = y + core if axis == "x" else x + y + core
    elif piece == 1:
        bit = y + core if axis == "z" else y + z + core
    else:
        bit = core if axis == "z" else z + core
    return 1 - 2 * wrap(bit, 2)


def locate(piece, kz, kx, dy, me, core):
    source = list(me)
    for axis in AXES[piece]:
        if axis == "y" and dy:
            source[2] = 1 - me[2]
        elif axis == "z" and kz:
            way = side(piece, axis, source, core)
            source[0] = wrap(me[0] + NZ + (-way * kz if kz <= 4 else way * (kz - 4)), NZ)
        elif axis == "x" and kx:
            way = side(piece, axis, source, core)
            source[1] = wrap(me[1] + NX + (-way * kx if kx <= 2 else way), NX)
    return tuple(source)


def moved(place, axis, step):
    z, x, y = place
    if axis == "z":
        return wrap(z + step + NZ, NZ), x, y
    if axis == "x":
        return z, wrap(x + step + NX, NX), y
    return z, x, 1 - y


def gather_schedule(me, core, start, take):
    for number, item in enumerate(PROGRAM):
        what, piece, kz, kx, dy = decode(item)
        if what == 9:
            if number in ENDS:
                take(ENDS[number])
        else:
            source = locate(piece, kz, kx, dy, me, core)
            short = what in (3, 5)
            if what:
                axis = {1: "y", 2: "z", 3: "z", 4: "x", 5: "x", 6: "z"}[what]
            else:
                places = {"z": kz, "x": kx, "y": dy}
                axis = [axis for axis in AXES[piece] if places[axis]][-1]
                short = axis == "z" and kz > 4
            way = side(piece, axis, source, core) if axis != "y" else 1
            start(piece, source, moved(me, axis, -way if short else way), SLOTS[receiver(what, piece, kz, kx, dy)])
        yield number


def receiver(what, piece, kz, kx, dy):
    if what == 0:
        if [axis for axis in AXES[piece] if {"z": kz, "x": kx, "y": dy}[axis]][-1] == "z":
            return piece, kz + 1, kx, dy
        return piece, kz, kx + 1, dy
    if what == 1:
        return piece, kz, kx, 1
    if what in (2, 3):
        return piece, 1 if what == 2 else 5, kx, dy
    if what in (4, 5):
        return piece, kz, 1 if what == 4 else 3, dy
    return piece, 4, kx, dy


def receive_slots(together):
    keys = {decode(item)[1:] for item in PROGRAM if item // 10000 != 9}
    slots, ends, last = {}, {}, []
    count = 0
    for number, item in enumerate(PROGRAM):
        what, *key = decode(item)
        key = tuple(key)
        if what != 9:
            continue
        if key in keys:
            slots[key] = count
            ends[number] = [key]
            count += 1
            continue
        last.append((number, key))
        if len(last) == together:
            ends[number] = [key for _, key in last]
            for _, key in last:
                slots[key] = count
            count += 1
            last = []
    if last:
        ends[last[-1][0]] = [key for _, key in last]
        for _, key in last:
            slots[key] = count
        count += 1
    return slots, ends, count


def index_of(place):
    return place[0] * PLANE + place[1] * NY + place[2]


PLANE = NX * NY
SENT = 63
CHUNK = 1024
TURN_ORDER = (0, 1, 2, 3, 7, 5, 6, 4)
TOGETHER = 4
SLOTS, ENDS, SLOT_COUNT = receive_slots(TOGETHER)
MIX_FROM = 110
MIX_STEP = 3


def kernel(
    a_hbm, l_hbm, mask_hbm, owner_hbm, dinv_hbm,
    panel_ref, upper_ref, diag_ref,
    whole, own, other, total, turned, mask_ref, owner_ref, dinv_ref,
    load_sem, send_sem, recv_sem, turn_send, turn_recv,
):
    leaf, here = lax.axis_index("leaf"), lax.axis_index("grid")
    core = lax.rem(leaf, 2)
    sibling = leaf + 1 - 2 * core
    me = (here // PLANE, lax.rem(here // NY, NX), lax.rem(here, NY))

    mine = pltpu.make_async_copy(
        l_hbm.at[0], whole.at[pl.ds(pl.multiple_of(here * ROWS, ROWS), ROWS)], load_sem.at[0]
    )
    mine.start()

    barrier = pltpu.get_barrier_semaphore()
    pl.semaphore_signal(barrier, inc=1, device_id=(sibling, here), device_id_type=MESH)
    for axis, way in WAYS:
        pl.semaphore_signal(
            barrier, inc=1, device_id=(leaf, index_of(moved(me, axis, way))), device_id_type=MESH
        )
    small = [
        pltpu.make_async_copy(mask_hbm, mask_ref, load_sem.at[1]),
        pltpu.make_async_copy(owner_hbm, owner_ref, load_sem.at[2]),
        pltpu.make_async_copy(dinv_hbm.at[0], dinv_ref, load_sem.at[3]),
    ]
    for copy in small:
        copy.start()
    pl.semaphore_wait(barrier, 1 + len(WAYS))
    mine.wait()

    def start(piece, source, place, slot):
        block = whole.at[
            pl.ds(pl.multiple_of(index_of(source) * ROWS + FIRST[piece], 16), COUNT[piece])
        ]
        pltpu.make_async_remote_copy(
            src_ref=block,
            dst_ref=block,
            send_sem=send_sem.at[piece],
            recv_sem=recv_sem.at[slot],
            device_id=(leaf, index_of(place)),
            device_id_type=MESH,
        ).start()

    def take(places):
        rows = whole.at[pl.ds(0, sum(COUNT[place[0]] for place in places))]
        pltpu.make_async_remote_copy(
            src_ref=rows, dst_ref=rows, send_sem=send_sem.at[0], recv_sem=recv_sem.at[SLOTS[places[0]]],
            device_id=(sibling, here), device_id_type=MESH,
        ).wait_recv()

    def multiply(blocks):
        product = None
        for block in blocks:
            number = moved(me, "z", block // NX)[0] * NX + moved(me, "x", block % NX)[1]
            columns = pl.ds(pl.multiple_of(number * B, B), B)
            part = jnp.dot(own[:, columns], whole[columns, :], preferred_element_type=jnp.float32)
            product = part if product is None else product + part
        total[...] += product

    def mix(first, count):
        def one(number, carry):
            columns = pl.ds(pl.multiple_of(number * B, B), B)
            swap = jnp.full((ROWS, B), owner_ref[number], jnp.int32) == 1
            keep = jnp.full((ROWS, B), mask_ref[number], jnp.int32) == 1
            mixed = jnp.where(swap, other[:, columns], own[:, columns])
            own[:, columns] = jnp.where(keep, mixed, jnp.zeros((), jnp.bfloat16))
            return carry

        lax.fori_loop(first, first + count, one, 0)

    def load(columns):
        return pltpu.make_async_copy(a_hbm.at[0, :, columns], own.at[:, columns], load_sem.at[4])

    def swap(columns):
        return pltpu.make_async_remote_copy(
            src_ref=a_hbm.at[0, :, columns],
            dst_ref=other.at[:, columns],
            send_sem=load_sem.at[5],
            recv_sem=load_sem.at[6],
            device_id=(sibling, here),
            device_id_type=MESH,
        )

    total[...] = jnp.zeros_like(total)
    issued, mixed = 0, 0
    for number in gather_schedule(me, core, start, take):
        if number % 4 == 3 and issued < SEP // CHUNK:
            columns = pl.ds(issued * CHUNK, CHUNK)
            load(columns).start()
            swap(columns).start()
            issued += 1
        if number == MIX_FROM:
            everything = pl.ds(0, SEP)
            for copy in small[:2] + [load(everything), swap(everything)]:
                copy.wait()
        if number >= MIX_FROM and (number - MIX_FROM) % MIX_STEP == 0 and mixed < SEP // B:
            mix(mixed, 2)
            mixed += 2
        if number in SITES:
            multiply(SITES[number])

    panel = (-total[...]).astype(jnp.bfloat16)
    turned[...] = panel.astype(jnp.float32).T.reshape(NGRID, B // NGRID, ROWS).astype(jnp.bfloat16)
    panel_ref[0] = panel

    rows_in = upper_ref.at[0]

    def column(place):
        return pl.ds(pl.multiple_of(place * ROWS, ROWS), ROWS)

    def turn(block, source, target):
        return pltpu.make_async_remote_copy(
            src_ref=block,
            dst_ref=rows_in.at[:, column(source)],
            send_sem=turn_send.at[0],
            recv_sem=turn_recv.at[source // PLANE],
            device_id=(leaf, target),
            device_id_type=MESH,
        )

    for plane in TURN_ORDER:
        for i in range(PLANE):
            target = plane * PLANE + lax.rem(here + i, PLANE)
            send = turn(turned.at[target], here, target)
            if i:
                send.start()
            else:
                pl.when(plane != me[0])(send.start)
    rows_in[:, column(here)] = turned[here]
    for piece in range(3):
        rows = whole.at[pl.ds(0, SENT * COUNT[piece])]
        pltpu.make_async_remote_copy(
            src_ref=rows, dst_ref=rows, send_sem=send_sem.at[piece], recv_sem=recv_sem.at[0],
            device_id=(sibling, here), device_id_type=MESH,
        ).wait_send()

    update = jnp.zeros((B // NGRID, B), jnp.float32)
    for dz in (0, 1, 7, 2, 6, 3, 5, 4):
        plane = moved(me, "z", dz)[0]
        count = PLANE if dz else PLANE - 1
        arrived = rows_in.at[:, pl.ds(0, count * ROWS)]
        pltpu.make_async_remote_copy(
            src_ref=arrived, dst_ref=arrived, send_sem=turn_send.at[0], recv_sem=turn_recv.at[plane],
            device_id=(sibling, here), device_id_type=MESH,
        ).wait_recv()
        for i in range(PLANE // NY):
            number = plane * (PLANE // NY) + i
            columns = pl.ds(pl.multiple_of(number * B, B), B)
            keep = jnp.full((B // NGRID, B), mask_ref[number], jnp.int32) == 1
            left = jnp.where(keep, rows_in[:, columns], jnp.zeros((), jnp.bfloat16))
            update += jnp.dot(left, whole[columns, :], preferred_element_type=jnp.float32)
    small[2].wait()
    diag_ref[0] = dinv_ref[...] - update

    direct = turned.at[pl.ds(0, NGRID - 1)]
    pltpu.make_async_remote_copy(
        src_ref=direct, dst_ref=direct, send_sem=turn_send.at[0], recv_sem=turn_recv.at[0],
        device_id=(sibling, here), device_id_type=MESH,
    ).wait_send()


def put_out(panel_ref, upper_ref, diag_ref, panel_out, upper_out, diag_out, sem):
    pairs = ((panel_ref, panel_out), (upper_ref, upper_out), (diag_ref, diag_out))
    copies = [pltpu.make_async_copy(a, b, sem.at[i]) for i, (a, b) in enumerate(pairs)]
    for copy in copies:
        copy.start()
    for copy in copies:
        copy.wait()


def body(ainv_sep, l_panel, block_mask, owner, dinv):
    vmem = pl.BlockSpec(memory_space=pltpu.VMEM)
    hbm = pl.BlockSpec(memory_space=pl.ANY)
    dma = pltpu.SemaphoreType.DMA
    shapes = (
        ((1, ROWS, B), jnp.bfloat16),
        ((1, B // NGRID, SEP), jnp.bfloat16),
        ((1, B // NGRID, B), jnp.float32),
    )
    results = pl.pallas_call(
        kernel,
        out_shape=tuple(pltpu.VMEM(*shape) for shape in shapes),
        in_specs=[hbm] * 5,
        out_specs=(vmem, vmem, vmem),
        scratch_shapes=[
            pltpu.VMEM((SEP, B), jnp.bfloat16),
            pltpu.VMEM((ROWS, SEP), jnp.bfloat16),
            pltpu.VMEM((ROWS, SEP), jnp.bfloat16),
            pltpu.VMEM((ROWS, B), jnp.float32),
            pltpu.VMEM((NGRID, B // NGRID, ROWS), jnp.bfloat16),
            pltpu.SMEM((SEP // B,), jnp.int32),
            pltpu.SMEM((SEP // B,), jnp.int32),
            pltpu.VMEM((B // NGRID, B), jnp.float32),
            dma((7,)),
            dma((3,)),
            dma((SLOT_COUNT,)),
            dma((1,)),
            dma((NZ,)),
        ],
        compiler_params=pltpu.CompilerParams(
            collective_id=0, has_side_effects=True, vmem_limit_bytes=60 * 1024 * 1024
        ),
    )(ainv_sep, l_panel, block_mask.reshape(-1), owner.reshape(-1), dinv)
    results = [pltpu.with_memory_space_constraint(result, pltpu.VMEM) for result in results]
    return pl.pallas_call(
        put_out,
        out_shape=tuple(jax.ShapeDtypeStruct(*shape) for shape in shapes),
        in_specs=[vmem] * 3,
        out_specs=(hbm, hbm, hbm),
        scratch_shapes=[dma((3,))],
    )(*results)


def solution(mesh):
    rows = P("leaf", "grid", None)
    return jax.shard_map(
        body,
        mesh=mesh,
        in_specs=(rows, rows, P("leaf", None, None), P("leaf", None), rows),
        out_specs=(rows, rows, rows),
        check_vma=False,
    )
```

```python
import functools

import jax
import jax.numpy as jnp
from jax import lax
from jax.experimental import pallas as pl
from jax.experimental.pallas import tpu as pltpu
from jax.sharding import PartitionSpec as P

MESH = pl.DeviceIdType.MESH
B = 512
SEP = 16384
ROWS = 256
NZ, NX, NY = 8, 4, 2
NGRID = NZ * NX * NY
WAYS = (("z", 1), ("z", -1), ("x", 1), ("x", -1), ("y", 1))

FIRST = (0, 80, 160)
COUNT = (80, 80, 96)
AXES = ("yxz", "yzx", "zxy")
PROGRAM = (
    22000, 32000, 42000, 52000, 12000, 10000, 21000, 31000, 50000, 40000, 11000, 20000, 30000, 41000, 51000,
    92001, 92500, 92100, 92030, 92010, 2500, 2100, 42100, 12100, 52500, 52100, 12500, 42500, 12030, 2010,
    12010, 90001, 91500, 91100, 90010, 90030, 1100, 20001, 1500, 20010, 50001, 40001, 20030, 10, 91001,
    90500, 90100, 91030, 91010, 31001, 21001, 92200, 92600, 52600, 2200, 2600, 12200, 42200, 52200, 12600,
    42600, 92530, 92101, 92110, 2110, 91200, 92501, 92130, 92510, 12510, 2510, 12110, 90101, 30010, 41100,
    1200, 91600, 92020, 92031, 90110, 12130, 30030, 90031, 20031, 90011, 20011, 11, 41500, 91501, 91101,
    1101, 90130, 30011, 30001, 92011, 12530, 90020, 20020, 92630, 92700, 42700, 92300, 42300, 52300, 2300,
    30031, 92201, 1501, 90111, 12020, 41001, 92210, 92230, 2210, 30020, 41200, 100, 92601, 12300, 90021,
    20021, 92610, 2610, 101, 91201, 41101, 52700, 90131, 92120, 92511, 41501, 130, 12610, 90120, 30021,
    1201, 92520, 41600, 110, 92111, 90510, 12210, 111, 91110, 90121, 91300, 41300, 92310, 92330, 90530,
    2310, 92131, 91510, 1600, 92400, 12700, 51100, 42400, 131, 90511, 90501, 41201, 500, 92531, 51500,
    12630, 92710, 120, 92620, 90531, 2710, 121, 91601, 91011, 92021, 530, 12230, 90520, 91210, 92220,
    90200, 41601, 501, 1010, 91111, 511, 92301, 90201, 12120, 92730, 52400, 1601, 51200, 510, 51001,
    91511, 531, 90230, 92611, 90521, 91301, 51101, 12520, 91310, 91610, 520, 90210, 200, 90211, 92211,
    51300, 12310, 201, 521, 91700, 41700, 51501, 92320, 41301, 91130, 92701, 92410, 90231, 12710, 230,
    91211, 90600, 2410, 51600, 91530, 90220, 211, 92631, 1301, 210, 12400, 90221, 51201, 92720, 90630,
    231, 1110, 92231, 91611, 12330, 600, 90601, 91020, 220, 90611, 1510, 51601, 91701, 41701, 91230,
    92121, 92430, 12620, 221, 90610, 91031, 601, 90631, 1011, 1210, 91131, 92521, 12220, 630, 90620,
    611, 1310, 90300, 1111, 91710, 91330, 61310, 92311, 610, 90301, 12730, 51301, 90621, 1511, 91531,
    91311, 631, 90330, 92711, 1300, 12410, 1610, 91630, 92420, 620, 90311, 91401, 41401, 300, 90310,
    91231, 1211, 92401, 51700, 12320, 301, 90331, 621, 91120, 91711, 51701, 1311, 92331, 90700, 12720,
    330, 90320, 311, 91520, 91631, 1611, 51401, 90321, 92621, 310, 90701, 12430, 91021, 91220, 331,
    1710, 1711, 90730, 61330, 92221, 321, 320, 90711, 12420, 91320, 91121, 91410, 1410, 90710, 91331,
    92731, 91521, 90731, 91400, 91411, 1411, 91620, 92411, 90720, 90400, 91221, 91730, 92321, 90401, 90721,
    91731, 91321, 90430, 90411, 92721, 91621, 91431, 90410, 90431, 92431, 91720, 91721, 91430, 90421, 90420,
    91421, 91420, 92421,
)
SITES = {
    160: (0, 4,),
    246: (28, 24,),
    277: (8, 1,),
    300: (3, 7, 29, 31,),
    325: (5, 9, 12, 20, 27, 25,),
    334: (11, 2,),
    347: (30, 6,),
    361: (21, 23, 16, 13,),
    365: (15, 10,),
    373: (26, 22, 19, 14,),
    377: (17, 18,),
}


def decode(item):
    return item // 10000, item // 1000 % 10, item // 100 % 10, item // 10 % 10, item % 10


def wrap(value, length):
    return value % length if isinstance(value, int) else lax.rem(value, length)


def side(piece, axis, source, core):
    z, x, y = source
    if piece == 0:
        bit = y + core if axis == "x" else x + y + core
    elif piece == 1:
        bit = y + core if axis == "z" else y + z + core
    else:
        bit = core if axis == "z" else z + core
    return 1 - 2 * wrap(bit, 2)


def locate(piece, kz, kx, dy, me, core):
    source = list(me)
    for axis in AXES[piece]:
        if axis == "y" and dy:
            source[2] = 1 - me[2]
        elif axis == "z" and kz:
            way = side(piece, axis, source, core)
            source[0] = wrap(me[0] + NZ + (-way * kz if kz <= 4 else way * (kz - 4)), NZ)
        elif axis == "x" and kx:
            way = side(piece, axis, source, core)
            source[1] = wrap(me[1] + NX + (-way * kx if kx <= 2 else way), NX)
    return tuple(source)


def moved(place, axis, step):
    z, x, y = place
    if axis == "z":
        return wrap(z + step + NZ, NZ), x, y
    if axis == "x":
        return z, wrap(x + step + NX, NX), y
    return z, x, 1 - y


def gather_schedule(me, core, start, take):
    for number, item in enumerate(PROGRAM):
        what, piece, kz, kx, dy = decode(item)
        if what == 9:
            if number in ENDS:
                take(ENDS[number])
        else:
            source = locate(piece, kz, kx, dy, me, core)
            short = what in (3, 5)
            if what:
                axis = {1: "y", 2: "z", 3: "z", 4: "x", 5: "x", 6: "z"}[what]
            else:
                places = {"z": kz, "x": kx, "y": dy}
                axis = [axis for axis in AXES[piece] if places[axis]][-1]
                short = axis == "z" and kz > 4
            way = side(piece, axis, source, core) if axis != "y" else 1
            start(piece, source, moved(me, axis, -way if short else way), SLOTS[receiver(what, piece, kz, kx, dy)])
        yield number


def receiver(what, piece, kz, kx, dy):
    if what == 0:
        if [axis for axis in AXES[piece] if {"z": kz, "x": kx, "y": dy}[axis]][-1] == "z":
            return piece, kz + 1, kx, dy
        return piece, kz, kx + 1, dy
    if what == 1:
        return piece, kz, kx, 1
    if what in (2, 3):
        return piece, 1 if what == 2 else 5, kx, dy
    if what in (4, 5):
        return piece, kz, 1 if what == 4 else 3, dy
    return piece, 4, kx, dy


def receive_slots(together):
    keys = {decode(item)[1:] for item in PROGRAM if item // 10000 != 9}
    slots, ends, last = {}, {}, []
    count = 0
    for number, item in enumerate(PROGRAM):
        what, *key = decode(item)
        key = tuple(key)
        if what != 9:
            continue
        if key in keys:
            slots[key] = count
            ends[number] = [key]
            count += 1
            continue
        last.append((number, key))
        if len(last) == together:
            ends[number] = [key for _, key in last]
            for _, key in last:
                slots[key] = count
            count += 1
            last = []
    if last:
        ends[last[-1][0]] = [key for _, key in last]
        for _, key in last:
            slots[key] = count
        count += 1
    return slots, ends, count


def index_of(place):
    return place[0] * PLANE + place[1] * NY + place[2]


PLANE = NX * NY
SENT = 63
CHUNK = 1024
TURN_ORDER = (0, 1, 2, 3, 7, 5, 6, 4)
TOGETHER = 4
SLOTS, ENDS, SLOT_COUNT = receive_slots(TOGETHER)
MIX_FROM = 110
MIX_STEP = 3


def kernel(
    a_hbm, l_hbm, mask_hbm, owner_hbm, dinv_hbm,
    panel_ref, upper_ref, diag_ref,
    whole, own, other, total, turned, mask_ref, owner_ref, dinv_ref,
    load_sem, send_sem, recv_sem, turn_send, turn_recv,
):
    leaf, here = lax.axis_index("leaf"), lax.axis_index("grid")
    core = lax.rem(leaf, 2)
    sibling = leaf + 1 - 2 * core
    me = (here // PLANE, lax.rem(here // NY, NX), lax.rem(here, NY))

    mine = pltpu.make_async_copy(
        l_hbm.at[0], whole.at[pl.ds(pl.multiple_of(here * ROWS, ROWS), ROWS)], load_sem.at[0]
    )
    mine.start()

    barrier = pltpu.get_barrier_semaphore()
    pl.semaphore_signal(barrier, inc=1, device_id=(sibling, here), device_id_type=MESH)
    for axis, way in WAYS:
        pl.semaphore_signal(
            barrier, inc=1, device_id=(leaf, index_of(moved(me, axis, way))), device_id_type=MESH
        )
    small = [
        pltpu.make_async_copy(mask_hbm, mask_ref, load_sem.at[1]),
        pltpu.make_async_copy(owner_hbm, owner_ref, load_sem.at[2]),
        pltpu.make_async_copy(dinv_hbm.at[0], dinv_ref, load_sem.at[3]),
    ]
    for copy in small:
        copy.start()
    pl.semaphore_wait(barrier, 1 + len(WAYS))
    mine.wait()

    def start(piece, source, place, slot):
        block = whole.at[
            pl.ds(pl.multiple_of(index_of(source) * ROWS + FIRST[piece], 16), COUNT[piece])
        ]
        pltpu.make_async_remote_copy(
            src_ref=block,
            dst_ref=block,
            send_sem=send_sem.at[piece],
            recv_sem=recv_sem.at[slot],
            device_id=(leaf, index_of(place)),
            device_id_type=MESH,
        ).start()

    def take(places):
        rows = whole.at[pl.ds(0, sum(COUNT[place[0]] for place in places))]
        pltpu.make_async_remote_copy(
            src_ref=rows, dst_ref=rows, send_sem=send_sem.at[0], recv_sem=recv_sem.at[SLOTS[places[0]]],
            device_id=(sibling, here), device_id_type=MESH,
        ).wait_recv()

    def multiply(blocks):
        product = None
        for block in blocks:
            number = moved(me, "z", block // NX)[0] * NX + moved(me, "x", block % NX)[1]
            columns = pl.ds(pl.multiple_of(number * B, B), B)
            part = jnp.dot(own[:, columns], whole[columns, :], preferred_element_type=jnp.float32)
            product = part if product is None else product + part
        total[...] += product

    def mix(first, count):
        def one(number, carry):
            columns = pl.ds(pl.multiple_of(number * B, B), B)
            swap = jnp.full((ROWS, B), owner_ref[number], jnp.int32) == 1
            keep = jnp.full((ROWS, B), mask_ref[number], jnp.int32) == 1
            mixed = jnp.where(swap, other[:, columns], own[:, columns])
            own[:, columns] = jnp.where(keep, mixed, jnp.zeros((), jnp.bfloat16))
            return carry

        lax.fori_loop(first, first + count, one, 0)

    def load(columns):
        return pltpu.make_async_copy(a_hbm.at[0, :, columns], own.at[:, columns], load_sem.at[4])

    def swap(columns):
        return pltpu.make_async_remote_copy(
            src_ref=a_hbm.at[0, :, columns],
            dst_ref=other.at[:, columns],
            send_sem=load_sem.at[5],
            recv_sem=load_sem.at[6],
            device_id=(sibling, here),
            device_id_type=MESH,
        )

    total[...] = jnp.zeros_like(total)
    issued, mixed = 0, 0
    for number in gather_schedule(me, core, start, take):
        if number % 4 == 3 and issued < SEP // CHUNK:
            columns = pl.ds(issued * CHUNK, CHUNK)
            load(columns).start()
            swap(columns).start()
            issued += 1
        if number == MIX_FROM:
            everything = pl.ds(0, SEP)
            for copy in small[:2] + [load(everything), swap(everything)]:
                copy.wait()
        if number >= MIX_FROM and (number - MIX_FROM) % MIX_STEP == 0 and mixed < SEP // B:
            mix(mixed, 2)
            mixed += 2
        if number in SITES:
            multiply(SITES[number])

    panel = (-total[...]).astype(jnp.bfloat16)
    turned[...] = panel.astype(jnp.float32).T.reshape(NGRID, B // NGRID, ROWS).astype(jnp.bfloat16)
    panel_ref[0] = panel

    rows_in = upper_ref.at[0]

    def column(place):
        return pl.ds(pl.multiple_of(place * ROWS, ROWS), ROWS)

    def turn(block, source, target):
        return pltpu.make_async_remote_copy(
            src_ref=block,
            dst_ref=rows_in.at[:, column(source)],
            send_sem=turn_send.at[0],
            recv_sem=turn_recv.at[source // PLANE],
            device_id=(leaf, target),
            device_id_type=MESH,
        )

    for plane in TURN_ORDER:
        for i in range(PLANE):
            target = plane * PLANE + lax.rem(here + i, PLANE)
            send = turn(turned.at[target], here, target)
            if i:
                send.start()
            else:
                pl.when(plane != me[0])(send.start)
    rows_in[:, column(here)] = turned[here]
    for piece in range(3):
        rows = whole.at[pl.ds(0, SENT * COUNT[piece])]
        pltpu.make_async_remote_copy(
            src_ref=rows, dst_ref=rows, send_sem=send_sem.at[piece], recv_sem=recv_sem.at[0],
            device_id=(sibling, here), device_id_type=MESH,
        ).wait_send()

    update = jnp.zeros((B // NGRID, B), jnp.float32)
    for dz in (0, 1, 7, 2, 6, 3, 5, 4):
        plane = moved(me, "z", dz)[0]
        count = PLANE if dz else PLANE - 1
        arrived = rows_in.at[:, pl.ds(0, count * ROWS)]
        pltpu.make_async_remote_copy(
            src_ref=arrived, dst_ref=arrived, send_sem=turn_send.at[0], recv_sem=turn_recv.at[plane],
            device_id=(sibling, here), device_id_type=MESH,
        ).wait_recv()
        columns = pl.ds(pl.multiple_of(plane * (PLANE * ROWS), B), PLANE * ROWS)
        parts = []
        for i in range(PLANE // NY):
            number = plane * (PLANE // NY) + i
            block = pl.ds(pl.multiple_of(number * B, B), B)
            keep = jnp.full((B // NGRID, B), mask_ref[number], jnp.int32) == 1
            parts.append(jnp.where(keep, rows_in[:, block], jnp.zeros((), jnp.bfloat16)))
        left = jnp.concatenate(parts, axis=1)
        update += jnp.dot(left, whole[columns, :], preferred_element_type=jnp.float32)
    small[2].wait()
    diag_ref[0] = dinv_ref[...] - update

    direct = turned.at[pl.ds(0, NGRID - 1)]
    pltpu.make_async_remote_copy(
        src_ref=direct, dst_ref=direct, send_sem=turn_send.at[0], recv_sem=turn_recv.at[0],
        device_id=(sibling, here), device_id_type=MESH,
    ).wait_send()


def put_out(panel_ref, upper_ref, diag_ref, panel_out, upper_out, diag_out, sem):
    pairs = ((panel_ref, panel_out), (upper_ref, upper_out), (diag_ref, diag_out))
    copies = [pltpu.make_async_copy(a, b, sem.at[i]) for i, (a, b) in enumerate(pairs)]
    for copy in copies:
        copy.start()
    for copy in copies:
        copy.wait()


def body(ainv_sep, l_panel, block_mask, owner, dinv):
    vmem = pl.BlockSpec(memory_space=pltpu.VMEM)
    hbm = pl.BlockSpec(memory_space=pl.ANY)
    dma = pltpu.SemaphoreType.DMA
    shapes = (
        ((1, ROWS, B), jnp.bfloat16),
        ((1, B // NGRID, SEP), jnp.bfloat16),
        ((1, B // NGRID, B), jnp.float32),
    )
    results = pl.pallas_call(
        kernel,
        out_shape=tuple(pltpu.VMEM(*shape) for shape in shapes),
        in_specs=[hbm] * 5,
        out_specs=(vmem, vmem, vmem),
        scratch_shapes=[
            pltpu.VMEM((SEP, B), jnp.bfloat16),
            pltpu.VMEM((ROWS, SEP), jnp.bfloat16),
            pltpu.VMEM((ROWS, SEP), jnp.bfloat16),
            pltpu.VMEM((ROWS, B), jnp.float32),
            pltpu.VMEM((NGRID, B // NGRID, ROWS), jnp.bfloat16),
            pltpu.SMEM((SEP // B,), jnp.int32),
            pltpu.SMEM((SEP // B,), jnp.int32),
            pltpu.VMEM((B // NGRID, B), jnp.float32),
            dma((7,)),
            dma((3,)),
            dma((SLOT_COUNT,)),
            dma((1,)),
            dma((NZ,)),
        ],
        compiler_params=pltpu.CompilerParams(
            collective_id=0, has_side_effects=True, vmem_limit_bytes=60 * 1024 * 1024
        ),
    )(ainv_sep, l_panel, block_mask.reshape(-1), owner.reshape(-1), dinv)
    results = [pltpu.with_memory_space_constraint(result, pltpu.VMEM) for result in results]
    return pl.pallas_call(
        put_out,
        out_shape=tuple(jax.ShapeDtypeStruct(*shape) for shape in shapes),
        in_specs=[vmem] * 3,
        out_specs=(hbm, hbm, hbm),
        scratch_shapes=[dma((3,))],
    )(*results)


def solution(mesh):
    rows = P("leaf", "grid", None)
    return jax.shard_map(
        body,
        mesh=mesh,
        in_specs=(rows, rows, P("leaf", None, None), P("leaf", None), rows),
        out_specs=(rows, rows, rows),
        check_vma=False,
    )
```
